32 devices in a mesh: plane: 8 (over z, x), wall: 4 (over y, core).
Axes of the slice: x: 2, y: 2, z: 4, core: 2. Of those that a mesh axis runs over, the one named last changes fastest.
Arguments:
- state: float32 [5, 125, 4, 1024], P(None, None, 'wall', 'plane'), may hold values from -6 to 6
- rhs: float32 [5, 125, 4, 1024], P(None, None, 'wall', 'plane'), may hold values from -6 to 6
- pivot_inv: float32 [125, 125, 4, 1024], P(None, None, 'wall', 'plane'), may hold values from -0.08944272 to 1.3394427
- coupling: float32 [125, 125, 4, 1024], P(None, None, 'wall', 'plane'), may hold values from -1.3 to 0.1
- face_coupling: float32 [4, 25, 25, 4, 1024], P(None, None, None, 'wall', 'plane'), may hold values from -1.25 to 1.25
- neighbors: int32 [1024, 4], P('plane'), may hold values from 0 to 1023, as said below
- counts: int32 [1024], P('plane'), may hold values from 2 to 4
Outputs:
- new_state: float32 [5, 125, 4, 1024], P(None, None, 'wall', 'plane')
- mean_square: float32 [], replicated
The draws below stay inside these ranges and needn't reach their ends.
Inputs may be any that keep to these rules, and one draw needn't show every extreme that they name: neighbors[l, f] is the line across face f of line l (0 next streamwise, 1 previous streamwise, 2 next spanwise, 3 previous spanwise); the relation is mutual with faces 0 and 1, and 2 and 3, paired. Line l lies on index l // 128 of plane; its neighbours across faces 2 and 3 lie on the same index, those across faces 0 and 1 on the same index or the next or previous one, wrapping around.
All inputs are finite; a program needn't handle non-finite values.
Results may differ from the reference program's by a relative error of at most 0.0001.
Values sent between devices are 32-bit elements; how exact they have to be, the bound alone decides.
A program may use at most 128 MiB of HBM per device.

```python
import math
import jax
import jax.numpy as jnp
from jax import lax

POINTS = 5
VARS = 5
DOFS = 125
FACE = 25
LINES_DEV = 128
STRIP = 4
ELEMS = 4
LINES = 1024


def line_rates(key):
    base = jax.random.fold_in(key, 4242)
    key_gain, key_slow, key_rate = jax.random.split(base, 3)
    gains = jnp.exp(jax.random.uniform(key_gain, (DOFS, ELEMS, LINES), jnp.float32, math.log(0.8), math.log(1.25)))
    share = 0.5
    slow = jax.random.uniform(key_slow, (DOFS, 1, LINES), jnp.float32) < share
    spread = jax.random.uniform(key_rate, (DOFS, ELEMS, LINES), jnp.float32)
    rates = jnp.where(slow, 0.85 + 0.08 * spread, 0.15 + 0.2 * spread)
    return (gains, rates)


def draw_pivot_inv(key, part):
    gains, rates = line_rates(key)
    noise = jnp.clip(jax.random.normal(jax.random.fold_in(key, 11), (DOFS, DOFS, ELEMS, LINES), jnp.float32), -4.0, 4.0)
    diagonal = jnp.eye(DOFS, dtype=jnp.float32)[:, :, None, None] * gains[None]
    return diagonal + noise * (0.25 / math.sqrt(DOFS))


def draw_coupling(key, part):
    gains, rates = line_rates(key)
    noise = jnp.clip(jax.random.normal(jax.random.fold_in(key, 12), (DOFS, DOFS, ELEMS, LINES), jnp.float32), -4.0, 4.0)
    diagonal = jnp.eye(DOFS, dtype=jnp.float32)[:, :, None, None] * (rates / gains)[None]
    return noise * (0.15 / math.sqrt(DOFS)) - diagonal


def draw_neighbors(key, part):
    plane_count = LINES // LINES_DEV
    span_count = LINES_DEV // STRIP
    keys = jax.random.split(jax.random.fold_in(key, 77), plane_count)
    slots = jax.vmap(lambda single: jax.random.permutation(single, LINES_DEV))(keys)
    ids = (jnp.arange(plane_count, dtype=jnp.int32)[:, None] * LINES_DEV + slots.astype(jnp.int32)).astype(jnp.int32)
    grid = ids.reshape(plane_count * STRIP, span_count)
    table = jnp.stack([jnp.roll(grid, -1, 0), jnp.roll(grid, 1, 0), jnp.roll(grid, -1, 1), jnp.roll(grid, 1, 1)], -1)
    table = table.reshape(-1, 4)
    result = jnp.zeros((LINES, 4), jnp.int32).at[grid.reshape(-1)].set(table)
    return result


def with_ends(values, rng, least, top_value):
    dims = values.shape
    place = [jax.random.randint(jax.random.fold_in(rng, axis), (), 0, dims[axis]) for axis in range(len(dims))]
    values = values.at[tuple(place)].set(least)
    longest = dims.index(max(dims))
    place[longest] = (place[longest] + 1) % dims[longest]
    return values.at[tuple(place)].set(top_value)


def steps_of(rng, extent, cuts, smallest, top_value):
    gain, own = 1.0, jax.random.fold_in(rng, 6)
    for dim, blocks in cuts:
        heights = jnp.exp(jax.random.uniform(jax.random.fold_in(own, dim), (blocks,), jnp.float32, smallest / len(cuts), top_value / len(cuts)))
        gain = gain * jnp.repeat(heights, extent[dim] // blocks).reshape([-1 if axis == dim else 1 for axis in range(len(extent))])
    return gain


def gaussian(stream_key, extent, scale, bound, cuts=(), held_as=jnp.bfloat16):
    entries = jax.random.normal(stream_key, extent, jnp.float32) * scale
    if len(cuts) > 0:
        entries = steps_of(stream_key, extent, cuts, -0.22, 0.18) * entries
    return jnp.clip(entries, min=-bound, max=bound).astype(held_as)


def setup_inputs(seed: int = 0) -> dict:
    streams_of = jax.random.split(jax.random.key(seed), 8)
    state = gaussian(streams_of[0], (VARS, DOFS, ELEMS, LINES), 1.0, 6.0, ((2, 4), (3, 8)), jnp.float32)
    rhs = gaussian(streams_of[1], (VARS, DOFS, ELEMS, LINES), 1.0, 6.0, ((2, 4), (3, 8)), jnp.float32)
    pivot_inv = draw_pivot_inv(jax.random.fold_in(streams_of[7], 71), 0)
    coupling = draw_coupling(jax.random.fold_in(streams_of[7], 71), 0)
    face_coupling = gaussian(streams_of[4], (4, FACE, FACE, ELEMS, LINES), FACE ** -0.5, 1.25, ((3, 4), (4, 8)), jnp.float32)
    neighbors = draw_neighbors(jax.random.fold_in(streams_of[7], 71), 0)
    counts = with_ends(jax.random.randint(streams_of[6], (LINES,), ELEMS // 2, ELEMS + 1), jax.random.fold_in(streams_of[6], 1), ELEMS // 2, ELEMS).astype(jnp.int32)
    return {"state": state, "rhs": rhs, "pivot_inv": pivot_inv, "coupling": coupling, "face_coupling": face_coupling, "neighbors": neighbors, "counts": counts}


highest = lax.Precision.HIGHEST
opposite = (1, 0, 3, 2)


def face_traces(state):
    tail = state.shape[2:]
    top_index = POINTS - 1
    cube = state.reshape((VARS, POINTS, POINTS, POINTS) + tail)
    faces = (cube[:, top_index], cube[:, 0], cube[:, :, :, top_index], cube[:, :, :, 0])
    return tuple(face.reshape((VARS, POINTS * POINTS) + tail) for face in faces)


def lift_faces(fluxes, tail):
    top_index = POINTS - 1
    cube = jnp.zeros((VARS, POINTS, POINTS, POINTS) + tail, jnp.float32)
    shaped = [flux.reshape((VARS, POINTS, POINTS) + tail) for flux in fluxes]
    cube = cube.at[:, top_index].add(shaped[0])
    cube = cube.at[:, 0].add(shaped[1])
    cube = cube.at[:, :, :, top_index].add(shaped[2])
    cube = cube.at[:, :, :, 0].add(shaped[3])
    return cube.reshape((VARS, POINTS * POINTS * POINTS) + tail)


def apply_block(block, vector):
    return jnp.einsum("jkl,vkl->vjl", block, vector, precision=highest)


def apply_transposed(block, vector):
    return jnp.einsum("kjl,vkl->vjl", block, vector, precision=highest)


def reference(state, rhs, pivot_inv, coupling, face_coupling, neighbors, counts):
    traces = face_traces(state)
    fluxes = []
    for face in range(4):
        received = jnp.take(traces[opposite[face]], neighbors[:, face], axis=3)
        fluxes.append(jnp.einsum("mnel,vnel->vmel", face_coupling[face], received, precision=highest))
    residual = rhs - lift_faces(fluxes, state.shape[2:])
    mean_square = jnp.mean(residual * residual)
    active = (jnp.arange(ELEMS)[:, None] < counts[None, :]).astype(jnp.float32)
    carried = jnp.zeros((VARS, DOFS, LINES), jnp.float32)
    forward = []
    for position in range(ELEMS):
        inner = residual[:, :, position] - apply_block(coupling[:, :, position], carried)
        carried = active[position] * apply_block(pivot_inv[:, :, position], inner)
        forward.append(carried)
    above = jnp.zeros((VARS, DOFS, LINES), jnp.float32)
    solved = [None] * ELEMS
    for position in reversed(range(ELEMS)):
        value = active[position] * (forward[position] - apply_block(pivot_inv[:, :, position], above))
        solved[position] = value
        above = apply_transposed(coupling[:, :, position], value)
    solution = jnp.stack(solved, axis=2)
    new_state = 0.2 * state + 0.8 * solution
    return new_state, mean_square
```

```python
import functools

import jax
import jax.numpy as jnp
from jax import lax
from jax.experimental import pallas as pl
from jax.experimental.pallas import tpu as pltpu
from jax.sharding import PartitionSpec as P

POINTS = 5
VARS = 5
DOFS = POINTS**3
FACE = POINTS**2
SUB = 8
TAIL = DOFS - SUB
GROUPS = -(-DOFS // SUB)
F32 = jnp.float32

STARTS = tuple(min(SUB * t, TAIL) for t in range(GROUPS))
FACE_STARTS = tuple(min(SUB * t, FACE - SUB) for t in range(-(-FACE // SUB)))
FACE_ROWS = ((DOFS - FACE, 1), (0, 1), (POINTS - 1, POINTS), (0, POINTS))


def sublanes():
    return lax.broadcasted_iota(jnp.int32, (SUB, 128), 0)


def row_sums(parts):
    sub = sublanes()

    def pair(x, y, shift):
        low = (sub & shift) == 0
        return jnp.where(low, x, y) + pltpu.roll(jnp.where(low, y, x), shift, 0)

    for shift in (1, 2, 4):
        parts = [pair(parts[i], parts[i + 1], shift) for i in range(0, len(parts), 2)]
    return parts[0]


def fresh_rows(tile, fresh):
    return jnp.where(sublanes() >= SUB - fresh, tile, 0.0)


def vector_tiles(load):
    tiles = [load(start) for start in STARTS]
    tiles[-1] = fresh_rows(tiles[-1], DOFS - SUB * (GROUPS - 1))
    return tiles


def apply_block(block, load, emit):
    tiles = vector_tiles(load)

    def group(g, carry):
        first = jnp.minimum(SUB * g, TAIL)
        parts = []
        for s in range(SUB):
            row = (first + s) * DOFS
            total = block[pl.ds(row, SUB), :] * tiles[0]
            for t in range(1, GROUPS):
                total = total + block[pl.ds(row + STARTS[t], SUB), :] * tiles[t]
            parts.append(total)
        emit(first, row_sums(parts))
        return carry

    lax.fori_loop(0, GROUPS, group, 0, unroll=2)


def apply_transposed(block, load_row, store):
    def step(j, totals):
        spread = jnp.broadcast_to(load_row(j), (SUB, 128))
        return tuple(
            totals[t] + block[pl.ds(j * DOFS + STARTS[t], SUB), :] * spread
            for t in range(GROUPS)
        )

    zeros = tuple(jnp.zeros((SUB, 128), F32) for _ in range(GROUPS))
    totals = lax.fori_loop(0, DOFS, step, zeros, unroll=5)
    for t in range(GROUPS):
        store(STARTS[t], totals[t])


def kernel(
    planes, walls, state, rhs, pivot, coupling, face, neighbors, counts, out, mean,
    st, r, pv, cp, fc, nb, ct, halo, fl, w, inner, below, x, back, above, fresh,
    ssq, plane_sums, wall_own, wall_sums,
    load_sem, out_sem, halo_send, halo_recv, fwd_send, fwd_recv, bwd_send, bwd_recv,
    plane_send, plane_recv, wall_send, wall_recv,
):
    me_p, me_w = lax.axis_index("plane"), lax.axis_index("wall")
    top = walls - 1

    loads = [
        pltpu.make_async_copy(state.at[:, :, 0, :], st.at[:, 0:DOFS, :], load_sem.at[0]),
        pltpu.make_async_copy(neighbors, nb, load_sem.at[1]),
        pltpu.make_async_copy(counts, ct, load_sem.at[2]),
        pltpu.make_async_copy(face.reshape(4 * FACE * FACE, 128), fc, load_sem.at[3]),
        pltpu.make_async_copy(rhs.at[:, :, 0, :], r.at[:, 0:DOFS, :], load_sem.at[4]),
    ]
    for load in loads:
        load.start()
    pivot_load = pltpu.make_async_copy(pivot.reshape(DOFS * DOFS, 128), pv, load_sem.at[5])
    coupling_load = pltpu.make_async_copy(
        coupling.reshape(DOFS * DOFS, 128), cp, load_sem.at[6]
    )

    barrier = pltpu.get_barrier_semaphore()
    for d in range(1, planes):
        pl.semaphore_signal(barrier, inc=1, device_id={"plane": lax.rem(me_p + d, planes)})
    for d in range(1, walls):
        pl.semaphore_signal(barrier, inc=1, device_id={"wall": lax.rem(me_w + d, walls)})

    pivot_load.start()

    @pl.when(me_w > 0)
    def _():
        coupling_load.start()

    pl.semaphore_wait(barrier, planes - 1 + walls - 1)

    def halo_copy(v, side, f):
        target = lax.rem(me_p + (1 if side == 0 else planes - 1), planes)
        return pltpu.make_async_remote_copy(
            src_ref=state.at[v, pl.ds(FACE_ROWS[f][0], FACE), 0, :],
            dst_ref=halo.at[v, side, f, 0:FACE, :],
            send_sem=halo_send.at[v, side, f],
            recv_sem=halo_recv.at[v, side, f],
            device_id={"plane": target},
        )

    def send_halo(v, carry):
        for side in range(2):
            for f in range(2):
                halo_copy(v, side, f).start()
        return carry

    lax.fori_loop(0, VARS, send_halo, 0)

    def fwd_copy(v):
        return pltpu.make_async_remote_copy(
            src_ref=w.at[v, 0:DOFS, :],
            dst_ref=below.at[v, 0:DOFS, :],
            send_sem=fwd_send.at[v],
            recv_sem=fwd_recv.at[v],
            device_id={"wall": lax.rem(me_w + 1, walls)},
        )

    def bwd_copy(v):
        return pltpu.make_async_remote_copy(
            src_ref=back.at[v, 0:DOFS, :],
            dst_ref=above.at[v, 0:DOFS, :],
            send_sem=bwd_send.at[v],
            recv_sem=bwd_recv.at[v],
            device_id={"wall": lax.rem(me_w + walls - 1, walls)},
        )

    def out_copy(v):
        return pltpu.make_async_copy(fresh.at[v, 0:DOFS, :], out.at[v, :, 0, :], out_sem.at[v])

    def plane_copy(d):
        return pltpu.make_async_remote_copy(
            src_ref=ssq,
            dst_ref=plane_sums.at[me_p],
            send_sem=plane_send.at[d],
            recv_sem=plane_recv.at[d],
            device_id={"plane": lax.rem(me_p + d, planes)},
        )

    def wall_copy(d):
        return pltpu.make_async_remote_copy(
            src_ref=wall_own,
            dst_ref=wall_sums.at[me_w],
            send_sem=wall_send.at[d],
            recv_sem=wall_recv.at[d],
            device_id={"wall": lax.rem(me_w + d, walls)},
        )

    ssq[...] = jnp.zeros((SUB, 128), F32)
    for load in loads:
        load.wait()
    active = jnp.broadcast_to(jnp.where(ct[...] > me_w, 1.0, 0.0).astype(F32), (SUB, 128))
    lane_bits = (st.shape[2] - 1).bit_length()

    def received_tiles(v, f):
        other = f ^ 1
        first, stride = FACE_ROWS[other]
        line = jnp.broadcast_to(nb[f : f + 1, :], (SUB, 128))
        slot = line & ((1 << lane_bits) - 1)
        away = (line >> lane_bits) - me_p
        here = away == 0
        before = (away == -1) | (away == planes - 1)

        def take(tile):
            return jnp.take_along_axis(tile, slot, axis=1, mode="promise_in_bounds")

        tiles = []
        for start in FACE_STARTS:
            if stride == 1:
                tile = take(st[v, pl.ds(first + start, SUB), :])
            else:
                tile = take(st[v, pl.ds(first + stride * start, SUB, stride=stride), :])
            if f < 2:
                low = take(halo[v, 0, other, pl.ds(start, SUB), :])
                high = take(halo[v, 1, other, pl.ds(start, SUB), :])
                tile = jnp.where(here, tile, jnp.where(before, low, high))
            tiles.append(tile)
        tiles[-1] = fresh_rows(tiles[-1], FACE - SUB * (len(FACE_STARTS) - 1))
        return tiles

    def residual(v):
        for f in (2, 3, 0, 1):
            if f == 0:
                for side in range(2):
                    for g in range(2):
                        halo_copy(v, side, g).wait_recv()
            tiles = received_tiles(v, f)

            def product(m):
                row = (f * FACE + m) * FACE
                total = fc[pl.ds(row, SUB), :] * tiles[0]
                for t in range(1, len(tiles)):
                    total = total + fc[pl.ds(row + FACE_STARTS[t], SUB), :] * tiles[t]
                return total

            whole = FACE // SUB * SUB
            for m in range(0, whole, SUB):
                fl[f, pl.ds(m, SUB), :] = row_sums([product(m + s) for s in range(SUB)])
            for m in range(whole, FACE):
                fl[f, pl.ds(m, 1), :] = jnp.sum(product(m), axis=0, keepdims=True)
        for f in range(4):
            first, stride = FACE_ROWS[f]
            rows = pl.ds(first, FACE) if stride == 1 else pl.ds(first, FACE, stride=stride)
            r[v, rows, :] = r[v, rows, :] - fl[f, 0:FACE, :]
        total = ssq[...]
        for tile in vector_tiles(lambda start: r[v, pl.ds(start, SUB), :]):
            total = total + tile * tile
        ssq[...] = total

    def forward(v, wall_element):
        if wall_element:
            source = lambda start: r[v, pl.ds(start, SUB), :]
        else:
            fwd_copy(v).wait_recv()

            def emit_inner(first, rows):
                inner[pl.ds(first, SUB), :] = r[v, pl.ds(first, SUB), :] - rows

            apply_block(cp, lambda start: below[v, pl.ds(start, SUB), :], emit_inner)
            source = lambda start: inner[pl.ds(start, SUB), :]

        def emit(first, rows):
            w[v, pl.ds(first, SUB), :] = active * rows

        apply_block(pv, source, emit)

        @pl.when(me_w < top)
        def _():
            fwd_copy(v).start()

    def send_down(v, source):
        def store(start, rows):
            back[v, pl.ds(start, SUB), :] = rows

        apply_transposed(cp, lambda j: source[v, pl.ds(j, 1), :], store)
        bwd_copy(v).start()

    def finish(v, source):
        for start in STARTS:
            rows = pl.ds(start, SUB)
            fresh[v, rows, :] = 0.2 * st[v, rows, :] + 0.8 * source[v, rows, :]
        out_copy(v).start()

    def first_loop(v, carry):
        residual(v)

        @pl.when(me_w == 0)
        def _():
            @pl.when(v == 0)
            def _():
                pivot_load.wait()

            forward(v, True)

        return carry

    lax.fori_loop(0, VARS, first_loop, 0)

    plane_sums[me_p] = ssq[...]
    for d in range(1, planes):
        plane_copy(d).start()

    @pl.when(me_w > 0)
    def _():
        pivot_load.wait()
        coupling_load.wait()

        def second_loop(v, carry):
            forward(v, False)

            @pl.when(me_w == top)
            def _():
                send_down(v, w)
                finish(v, w)

            return carry

        lax.fori_loop(0, VARS, second_loop, 0)

    for d in range(1, planes):
        plane_copy(d).wait()
    total = plane_sums[0]
    for i in range(1, planes):
        total = total + plane_sums[i]
    wall_own[...] = total
    wall_sums[me_w] = total
    for d in range(1, walls):
        wall_copy(d).start()

    @pl.when(me_w < top)
    def _():
        def third_loop(v, carry):
            bwd_copy(v).wait_recv()

            def emit(first, rows):
                x[v, pl.ds(first, SUB), :] = active * (w[v, pl.ds(first, SUB), :] - rows)

            apply_block(pv, lambda start: above[v, pl.ds(start, SUB), :], emit)

            @pl.when(me_w > 0)
            def _():
                send_down(v, x)

            finish(v, x)
            return carry

        lax.fori_loop(0, VARS, third_loop, 0)

    for d in range(1, walls):
        wall_copy(d).wait()
    total = wall_sums[0]
    for i in range(1, walls):
        total = total + wall_sums[i]
    mean[0, 0] = jnp.sum(total) / float(VARS * DOFS * 128 * planes * walls)

    def drain(v, carry):
        out_copy(v).wait()
        for side in range(2):
            for f in range(2):
                halo_copy(v, side, f).wait_send()

        @pl.when(me_w < top)
        def _():
            fwd_copy(v).wait_send()

        @pl.when(me_w > 0)
        def _():
            bwd_copy(v).wait_send()

        return carry

    lax.fori_loop(0, VARS, drain, 0)


def body(planes, walls, state, rhs, pivot_inv, coupling, face_coupling, neighbors, counts):
    lines = state.shape[3]
    assert state.shape[2] == 1 and lines == 128 and walls > 1
    rows = DOFS + 3
    face_rows = FACE + 7
    vectors = pltpu.VMEM((VARS, rows, lines), F32)
    dma = pltpu.SemaphoreType.DMA
    anywhere = pl.BlockSpec(memory_space=pl.ANY)
    new_state, mean = pl.pallas_call(
        functools.partial(kernel, planes, walls),
        out_shape=(
            jax.ShapeDtypeStruct(state.shape, F32),
            jax.ShapeDtypeStruct((1, 1), F32),
        ),
        in_specs=[anywhere] * 7,
        out_specs=(anywhere, pl.BlockSpec(memory_space=pltpu.SMEM)),
        scratch_shapes=[
            vectors,
            vectors,
            pltpu.VMEM((DOFS * DOFS, lines), F32),
            pltpu.VMEM((DOFS * DOFS, lines), F32),
            pltpu.VMEM((4 * FACE * FACE, lines), F32),
            pltpu.VMEM((4, lines), jnp.int32),
            pltpu.VMEM((1, lines), jnp.int32),
            pltpu.VMEM((VARS, 2, 2, face_rows, lines), F32),
            pltpu.VMEM((4, face_rows, lines), F32),
            vectors,
            pltpu.VMEM((rows, lines), F32),
            vectors,
            vectors,
            vectors,
            vectors,
            vectors,
            pltpu.VMEM((SUB, lines), F32),
            pltpu.VMEM((planes, SUB, lines), F32),
            pltpu.VMEM((SUB, lines), F32),
            pltpu.VMEM((walls, SUB, lines), F32),
            dma((7,)),
            dma((VARS,)),
            dma((VARS, 2, 2)),
            dma((VARS, 2, 2)),
            dma((VARS,)),
            dma((VARS,)),
            dma((VARS,)),
            dma((VARS,)),
            dma((planes,)),
            dma((planes,)),
            dma((walls,)),
            dma((walls,)),
        ],
        compiler_params=pltpu.CompilerParams(
            collective_id=0, has_side_effects=True, vmem_limit_bytes=40 * 2**20
        ),
        name="line_sweep",
    )(
        state, rhs, pivot_inv, coupling, face_coupling, neighbors.T, counts.reshape(1, lines)
    )
    return new_state, mean.reshape(())


def solution(mesh):
    planes, walls = mesh.shape["plane"], mesh.shape["wall"]
    field = P(None, None, "wall", "plane")
    return jax.shard_map(
        functools.partial(body, planes, walls),
        mesh=mesh,
        in_specs=(
            field, field, field, field,
            P(None, None, None, "wall", "plane"),
            P("plane", None),
            P("plane"),
        ),
        out_specs=(field, P()),
        check_vma=False,
    )
```

```python
import functools

import jax
import jax.numpy as jnp
from jax import lax
from jax.experimental import pallas as pl
from jax.experimental.pallas import tpu as pltpu
from jax.sharding import PartitionSpec as P

POINTS = 5
VARS = 5
DOFS = POINTS**3
FACE = POINTS**2
SUB = 8
TAIL = DOFS - SUB
GROUPS = -(-DOFS // SUB)
F32 = jnp.float32

STARTS = tuple(min(SUB * t, TAIL) for t in range(GROUPS))
FACE_STARTS = tuple(min(SUB * t, FACE - SUB) for t in range(-(-FACE // SUB)))
FACE_ROWS = ((DOFS - FACE, 1), (0, 1), (POINTS - 1, POINTS), (0, POINTS))


def sublanes():
    return lax.broadcasted_iota(jnp.int32, (SUB, 128), 0)


def row_sums(parts):
    sub = sublanes()

    def pair(x, y, shift):
        low = (sub & shift) == 0
        return jnp.where(low, x, y) + pltpu.roll(jnp.where(low, y, x), shift, 0)

    for shift in (1, 2, 4):
        parts = [pair(parts[i], parts[i + 1], shift) for i in range(0, len(parts), 2)]
    return parts[0]


def fresh_rows(tile, fresh):
    return jnp.where(sublanes() >= SUB - fresh, tile, 0.0)


def vector_tiles(load):
    tiles = [load(start) for start in STARTS]
    tiles[-1] = fresh_rows(tiles[-1], DOFS - SUB * (GROUPS - 1))
    return tiles


def apply_block(block, load, emit):
    tiles = vector_tiles(load)

    def group(g, carry):
        first = jnp.minimum(SUB * g, TAIL)
        parts = []
        for s in range(SUB):
            row = (first + s) * DOFS
            total = block[pl.ds(row, SUB), :] * tiles[0]
            for t in range(1, GROUPS):
                total = total + block[pl.ds(row + STARTS[t], SUB), :] * tiles[t]
            parts.append(total)
        emit(first, row_sums(parts))
        return carry

    lax.fori_loop(0, GROUPS, group, 0, unroll=2)


def apply_transposed(block, load_row, store):
    def step(j, totals):
        spread = jnp.broadcast_to(load_row(j), (SUB, 128))
        return tuple(
            totals[t] + block[pl.ds(j * DOFS + STARTS[t], SUB), :] * spread
            for t in range(GROUPS)
        )

    zeros = tuple(jnp.zeros((SUB, 128), F32) for _ in range(GROUPS))
    totals = lax.fori_loop(0, DOFS, step, zeros, unroll=25)
    for t in range(GROUPS):
        store(STARTS[t], totals[t])


def kernel(
    planes, walls, state, rhs, pivot, coupling, face, neighbors, counts, out, mean,
    st, r, pv, cp, fc, nb, ct, halo, fl, w, inner, below, x, back, above, fresh,
    ssq, plane_sums, wall_own, wall_sums,
    load_sem, out_sem, halo_send, halo_recv, fwd_send, fwd_recv, bwd_send, bwd_recv,
    plane_send, plane_recv, wall_send, wall_recv,
):
    me_p, me_w = lax.axis_index("plane"), lax.axis_index("wall")
    top = walls - 1

    loads = [
        pltpu.make_async_copy(state.at[:, :, 0, :], st.at[:, 0:DOFS, :], load_sem.at[0]),
        pltpu.make_async_copy(neighbors, nb, load_sem.at[1]),
        pltpu.make_async_copy(counts, ct, load_sem.at[2]),
        pltpu.make_async_copy(face.reshape(4 * FACE * FACE, 128), fc, load_sem.at[3]),
        pltpu.make_async_copy(rhs.at[:, :, 0, :], r.at[:, 0:DOFS, :], load_sem.at[4]),
    ]
    for load in loads:
        load.start()
    pivot_load = pltpu.make_async_copy(pivot.reshape(DOFS * DOFS, 128), pv, load_sem.at[5])
    coupling_load = pltpu.make_async_copy(
        coupling.reshape(DOFS * DOFS, 128), cp, load_sem.at[6]
    )

    barrier = pltpu.get_barrier_semaphore()
    for d in range(1, planes):
        pl.semaphore_signal(barrier, inc=1, device_id={"plane": lax.rem(me_p + d, planes)})
    for d in range(1, walls):
        pl.semaphore_signal(barrier, inc=1, device_id={"wall": lax.rem(me_w + d, walls)})

    pivot_load.start()

    @pl.when(me_w > 0)
    def _():
        coupling_load.start()

    pl.semaphore_wait(barrier, planes - 1 + walls - 1)

    def halo_copy(v, side, f):
        target = lax.rem(me_p + (1 if side == 0 else planes - 1), planes)
        return pltpu.make_async_remote_copy(
            src_ref=state.at[v, pl.ds(FACE_ROWS[f][0], FACE), 0, :],
            dst_ref=halo.at[v, side, f, 0:FACE, :],
            send_sem=halo_send.at[v, side, f],
            recv_sem=halo_recv.at[v, side, f],
            device_id={"plane": target},
        )

    def send_halo(v, carry):
        for side in range(2):
            for f in range(2):
                halo_copy(v, side, f).start()
        return carry

    lax.fori_loop(0, VARS, send_halo, 0)

    def fwd_copy(v):
        return pltpu.make_async_remote_copy(
            src_ref=w.at[v, 0:DOFS, :],
            dst_ref=below.at[v, 0:DOFS, :],
            send_sem=fwd_send.at[v],
            recv_sem=fwd_recv.at[v],
            device_id={"wall": lax.rem(me_w + 1, walls)},
        )

    def bwd_copy(v):
        return pltpu.make_async_remote_copy(
            src_ref=back.at[v, 0:DOFS, :],
            dst_ref=above.at[v, 0:DOFS, :],
            send_sem=bwd_send.at[v],
            recv_sem=bwd_recv.at[v],
            device_id={"wall": lax.rem(me_w + walls - 1, walls)},
        )

    def out_copy(v):
        return pltpu.make_async_copy(fresh.at[v, 0:DOFS, :], out.at[v, :, 0, :], out_sem.at[v])

    def plane_copy(d):
        return pltpu.make_async_remote_copy(
            src_ref=ssq,
            dst_ref=plane_sums.at[me_p],
            send_sem=plane_send.at[d],
            recv_sem=plane_recv.at[d],
            device_id={"plane": lax.rem(me_p + d, planes)},
        )

    def wall_copy(d):
        return pltpu.make_async_remote_copy(
            src_ref=wall_own,
            dst_ref=wall_sums.at[me_w],
            send_sem=wall_send.at[d],
            recv_sem=wall_recv.at[d],
            device_id={"wall": lax.rem(me_w + d, walls)},
        )

    ssq[...] = jnp.zeros((SUB, 128), F32)
    for load in loads:
        load.wait()
    active = jnp.broadcast_to(jnp.where(ct[...] > me_w, 1.0, 0.0).astype(F32), (SUB, 128))
    lane_bits = (st.shape[2] - 1).bit_length()

    def received_tiles(v, f):
        other = f ^ 1
        first, stride = FACE_ROWS[other]
        line = jnp.broadcast_to(nb[f : f + 1, :], (SUB, 128))
        slot = line & ((1 << lane_bits) - 1)
        away = (line >> lane_bits) - me_p
        here = away == 0
        before = (away == -1) | (away == planes - 1)

        def take(tile):
            return jnp.take_along_axis(tile, slot, axis=1, mode="promise_in_bounds")

        tiles = []
        for start in FACE_STARTS:
            if stride == 1:
                tile = take(st[v, pl.ds(first + start, SUB), :])
            else:
                tile = take(st[v, pl.ds(first + stride * start, SUB, stride=stride), :])
            if f < 2:
                low = take(halo[v, 0, other, pl.ds(start, SUB), :])
                high = take(halo[v, 1, other, pl.ds(start, SUB), :])
                tile = jnp.where(here, tile, jnp.where(before, low, high))
            tiles.append(tile)
        tiles[-1] = fresh_rows(tiles[-1], FACE - SUB * (len(FACE_STARTS) - 1))
        return tiles

    def residual(v):
        for f in (2, 3, 0, 1):
            if f == 0:
                for side in range(2):
                    for g in range(2):
                        halo_copy(v, side, g).wait_recv()
            tiles = received_tiles(v, f)

            def product(m):
                row = (f * FACE + m) * FACE
                total = fc[pl.ds(row, SUB), :] * tiles[0]
                for t in range(1, len(tiles)):
                    total = total + fc[pl.ds(row + FACE_STARTS[t], SUB), :] * tiles[t]
                return total

            whole = FACE // SUB * SUB
            for m in range(0, whole, SUB):
                fl[f, pl.ds(m, SUB), :] = row_sums([product(m + s) for s in range(SUB)])
            for m in range(whole, FACE):
                fl[f, pl.ds(m, 1), :] = jnp.sum(product(m), axis=0, keepdims=True)
        for f in range(4):
            first, stride = FACE_ROWS[f]
            rows = pl.ds(first, FACE) if stride == 1 else pl.ds(first, FACE, stride=stride)
            r[v, rows, :] = r[v, rows, :] - fl[f, 0:FACE, :]
        total = ssq[...]
        for tile in vector_tiles(lambda start: r[v, pl.ds(start, SUB), :]):
            total = total + tile * tile
        ssq[...] = total

    def forward(v, wall_element):
        if wall_element:
            source = lambda start: r[v, pl.ds(start, SUB), :]
        else:
            fwd_copy(v).wait_recv()

            def emit_inner(first, rows):
                inner[pl.ds(first, SUB), :] = r[v, pl.ds(first, SUB), :] - rows

            apply_block(cp, lambda start: below[v, pl.ds(start, SUB), :], emit_inner)
            source = lambda start: inner[pl.ds(start, SUB), :]

        def emit(first, rows):
            w[v, pl.ds(first, SUB), :] = active * rows

        apply_block(pv, source, emit)

        @pl.when(me_w < top)
        def _():
            fwd_copy(v).start()

    def send_down(v, source):
        def store(start, rows):
            back[v, pl.ds(start, SUB), :] = rows

        apply_transposed(cp, lambda j: source[v, pl.ds(j, 1), :], store)
        bwd_copy(v).start()

    def finish(v, source):
        for start in STARTS:
            rows = pl.ds(start, SUB)
            fresh[v, rows, :] = 0.2 * st[v, rows, :] + 0.8 * source[v, rows, :]
        out_copy(v).start()

    def first_loop(v, carry):
        residual(v)

        @pl.when(me_w == 0)
        def _():
            @pl.when(v == 0)
            def _():
                pivot_load.wait()

            forward(v, True)

        return carry

    lax.fori_loop(0, VARS, first_loop, 0)

    plane_sums[me_p] = ssq[...]
    for d in range(1, planes):
        plane_copy(d).start()

    @pl.when(me_w > 0)
    def _():
        pivot_load.wait()
        coupling_load.wait()

        def second_loop(v, carry):
            forward(v, False)

            @pl.when(me_w == top)
            def _():
                send_down(v, w)
                finish(v, w)

            return carry

        lax.fori_loop(0, VARS, second_loop, 0)

    for d in range(1, planes):
        plane_copy(d).wait()
    total = plane_sums[0]
    for i in range(1, planes):
        total = total + plane_sums[i]
    wall_own[...] = total
    wall_sums[me_w] = total
    for d in range(1, walls):
        wall_copy(d).start()

    @pl.when(me_w < top)
    def _():
        def third_loop(v, carry):
            bwd_copy(v).wait_recv()

            def emit(first, rows):
                x[v, pl.ds(first, SUB), :] = active * (w[v, pl.ds(first, SUB), :] - rows)

            apply_block(pv, lambda start: above[v, pl.ds(start, SUB), :], emit)

            @pl.when(me_w > 0)
            def _():
                send_down(v, x)

            finish(v, x)
            return carry

        lax.fori_loop(0, VARS, third_loop, 0)

    for d in range(1, walls):
        wall_copy(d).wait()
    total = wall_sums[0]
    for i in range(1, walls):
        total = total + wall_sums[i]
    mean[0, 0] = jnp.sum(total) / float(VARS * DOFS * 128 * planes * walls)

    def drain(v, carry):
        out_copy(v).wait()
        for side in range(2):
            for f in range(2):
                halo_copy(v, side, f).wait_send()

        @pl.when(me_w < top)
        def _():
            fwd_copy(v).wait_send()

        @pl.when(me_w > 0)
        def _():
            bwd_copy(v).wait_send()

        return carry

    lax.fori_loop(0, VARS, drain, 0)


def body(planes, walls, state, rhs, pivot_inv, coupling, face_coupling, neighbors, counts):
    lines = state.shape[3]
    assert state.shape[2] == 1 and lines == 128 and walls > 1
    rows = DOFS + 3
    face_rows = FACE + 7
    vectors = pltpu.VMEM((VARS, rows, lines), F32)
    dma = pltpu.SemaphoreType.DMA
    anywhere = pl.BlockSpec(memory_space=pltpu.HBM)
    new_state, mean = pl.pallas_call(
        functools.partial(kernel, planes, walls),
        out_shape=(
            jax.ShapeDtypeStruct(state.shape, F32),
            jax.ShapeDtypeStruct((1, 1), F32),
        ),
        in_specs=[anywhere] * 7,
        out_specs=(anywhere, pl.BlockSpec(memory_space=pltpu.SMEM)),
        scratch_shapes=[
            vectors,
            vectors,
            pltpu.VMEM((DOFS * DOFS, lines), F32),
            pltpu.VMEM((DOFS * DOFS, lines), F32),
            pltpu.VMEM((4 * FACE * FACE, lines), F32),
            pltpu.VMEM((4, lines), jnp.int32),
            pltpu.VMEM((1, lines), jnp.int32),
            pltpu.VMEM((VARS, 2, 2, face_rows, lines), F32),
            pltpu.VMEM((4, face_rows, lines), F32),
            vectors,
            pltpu.VMEM((rows, lines), F32),
            vectors,
            vectors,
            vectors,
            vectors,
            vectors,
            pltpu.VMEM((SUB, lines), F32),
            pltpu.VMEM((planes, SUB, lines), F32),
            pltpu.VMEM((SUB, lines), F32),
            pltpu.VMEM((walls, SUB, lines), F32),
            dma((7,)),
            dma((VARS,)),
            dma((VARS, 2, 2)),
            dma((VARS, 2, 2)),
            dma((VARS,)),
            dma((VARS,)),
            dma((VARS,)),
            dma((VARS,)),
            dma((planes,)),
            dma((planes,)),
            dma((walls,)),
            dma((walls,)),
        ],
        compiler_params=pltpu.CompilerParams(
            collective_id=0, has_side_effects=True, vmem_limit_bytes=67_043_328
        ),
        name="line_sweep",
    )(
        state, rhs, pivot_inv, coupling, face_coupling, neighbors.T, counts.reshape(1, lines)
    )
    return new_state, mean.reshape(())


def solution(mesh):
    planes, walls = mesh.shape["plane"], mesh.shape["wall"]
    field = P(None, None, "wall", "plane")
    return jax.shard_map(
        functools.partial(body, planes, walls),
        mesh=mesh,
        in_specs=(
            field, field, field, field,
            P(None, None, None, "wall", "plane"),
            P("plane", None),
            P("plane"),
        ),
        out_specs=(field, P()),
        check_vma=False,
    )
```

```python
import functools

import jax
import jax.numpy as jnp
from jax import lax
from jax.experimental import pallas as pl
from jax.experimental.pallas import tpu as pltpu
from jax.sharding import PartitionSpec as P

POINTS = 5
VARS = 5
DOFS = POINTS**3
FACE = POINTS**2
SUB = 8
TAIL = DOFS - SUB
GROUPS = -(-DOFS // SUB)
F32 = jnp.float32

STARTS = tuple(min(SUB * t, TAIL) for t in range(GROUPS))
FACE_STARTS = tuple(min(SUB * t, FACE - SUB) for t in range(-(-FACE // SUB)))
HALVES = (slice(0, SUB * (GROUPS // 2)), slice(SUB * (GROUPS // 2), DOFS))
FACE_ROWS = ((DOFS - FACE, 1), (0, 1), (POINTS - 1, POINTS), (0, POINTS))


def sublanes():
    return lax.broadcasted_iota(jnp.int32, (SUB, 128), 0)


def row_sums(parts):
    sub = sublanes()

    def pair(x, y, shift):
        low = (sub & shift) == 0
        return jnp.where(low, x, y) + pltpu.roll(jnp.where(low, y, x), shift, 0)

    for shift in (1, 2, 4):
        parts = [pair(parts[i], parts[i + 1], shift) for i in range(0, len(parts), 2)]
    return parts[0]


def fresh_rows(tile, fresh):
    return jnp.where(sublanes() >= SUB - fresh, tile, 0.0)


def vector_tiles(load):
    tiles = [load(start) for start in STARTS]
    tiles[-1] = fresh_rows(tiles[-1], DOFS - SUB * (GROUPS - 1))
    return tiles


def apply_block(block, load, emit, halfway=None):
    tiles = vector_tiles(load)

    def group(g, carry):
        first = jnp.minimum(SUB * g, TAIL)
        parts = []
        for s in range(SUB):
            row = (first + s) * DOFS
            total = block[pl.ds(row, SUB), :] * tiles[0]
            for t in range(1, GROUPS):
                total = total + block[pl.ds(row + STARTS[t], SUB), :] * tiles[t]
            parts.append(total)
        emit(first, row_sums(parts))
        return carry

    if halfway is None:
        lax.fori_loop(0, GROUPS, group, 0, unroll=4)
    else:
        lax.fori_loop(0, GROUPS // 2, group, 0, unroll=4)
        halfway()
        lax.fori_loop(GROUPS // 2, GROUPS, group, 0, unroll=4)


def apply_transposed(block, load_row, store, starts):
    def step(j, totals):
        spread = jnp.broadcast_to(load_row(j), (SUB, 128))
        return tuple(
            total + block[pl.ds(j * DOFS + start, SUB), :] * spread
            for total, start in zip(totals, starts)
        )

    zeros = tuple(jnp.zeros((SUB, 128), F32) for _ in starts)
    totals = lax.fori_loop(0, DOFS, step, zeros, unroll=25)
    for start, total in zip(starts, totals):
        store(start, total)


def kernel(
    planes, walls, state, rhs, pivot, coupling, face, neighbors, counts, out, mean,
    st, r, pv, cp, fc, nb, ct, halo, fl, w, inner, below, x, back, above, fresh,
    ssq, plane_sums, wall_own, wall_sums,
    load_sem, out_sem, halo_send, halo_recv, fwd_send, fwd_recv, bwd_send, bwd_recv,
    plane_send, plane_recv, wall_send, wall_recv,
):
    me_p, me_w = lax.axis_index("plane"), lax.axis_index("wall")
    top = walls - 1

    loads = [
        pltpu.make_async_copy(state.at[:, :, 0, :], st.at[:, 0:DOFS, :], load_sem.at[0]),
        pltpu.make_async_copy(neighbors, nb, load_sem.at[1]),
        pltpu.make_async_copy(counts, ct, load_sem.at[2]),
        pltpu.make_async_copy(face.reshape(4 * FACE * FACE, 128), fc, load_sem.at[3]),
        pltpu.make_async_copy(rhs.at[:, :, 0, :], r.at[:, 0:DOFS, :], load_sem.at[4]),
    ]
    for load in loads:
        load.start()
    pivot_load = pltpu.make_async_copy(pivot.reshape(DOFS * DOFS, 128), pv, load_sem.at[5])
    coupling_load = pltpu.make_async_copy(
        coupling.reshape(DOFS * DOFS, 128), cp, load_sem.at[6]
    )

    barrier = pltpu.get_barrier_semaphore()
    for d in range(1, planes):
        pl.semaphore_signal(barrier, inc=1, device_id={"plane": lax.rem(me_p + d, planes)})
    for d in range(1, walls):
        pl.semaphore_signal(barrier, inc=1, device_id={"wall": lax.rem(me_w + d, walls)})

    pivot_load.start()

    @pl.when(me_w > 0)
    def _():
        coupling_load.start()

    pl.semaphore_wait(barrier, planes - 1 + walls - 1)
    loads[0].wait()

    def halo_copy(v, side, f):
        target = lax.rem(me_p + (1 if side == 0 else planes - 1), planes)
        return pltpu.make_async_remote_copy(
            src_ref=st.at[v, pl.ds(FACE_ROWS[f][0], FACE), :],
            dst_ref=halo.at[v, side, f, 0:FACE, :],
            send_sem=halo_send.at[v, side, f],
            recv_sem=halo_recv.at[v, side, f],
            device_id={"plane": target},
        )

    def send_halo(v, carry):
        for side in range(2):
            for f in range(2):
                halo_copy(v, side, f).start()
        return carry

    lax.fori_loop(0, VARS, send_halo, 0)

    def fwd_copy(v, half):
        rows = HALVES[half]
        return pltpu.make_async_remote_copy(
            src_ref=w.at[v, rows, :],
            dst_ref=below.at[v, rows, :],
            send_sem=fwd_send.at[v, half],
            recv_sem=fwd_recv.at[v, half],
            device_id={"wall": lax.rem(me_w + 1, walls)},
        )

    def bwd_copy(v, half):
        rows = HALVES[half]
        return pltpu.make_async_remote_copy(
            src_ref=back.at[v, rows, :],
            dst_ref=above.at[v, rows, :],
            send_sem=bwd_send.at[v, half],
            recv_sem=bwd_recv.at[v, half],
            device_id={"wall": lax.rem(me_w + walls - 1, walls)},
        )

    def out_copy(v):
        return pltpu.make_async_copy(fresh.at[v, 0:DOFS, :], out.at[v, :, 0, :], out_sem.at[v])

    def plane_copy(d):
        return pltpu.make_async_remote_copy(
            src_ref=ssq,
            dst_ref=plane_sums.at[me_p],
            send_sem=plane_send.at[d],
            recv_sem=plane_recv.at[d],
            device_id={"plane": lax.rem(me_p + d, planes)},
        )

    def wall_copy(d):
        return pltpu.make_async_remote_copy(
            src_ref=wall_own,
            dst_ref=wall_sums.at[me_w],
            send_sem=wall_send.at[d],
            recv_sem=wall_recv.at[d],
            device_id={"wall": lax.rem(me_w + d, walls)},
        )

    ssq[...] = jnp.zeros((SUB, 128), F32)
    for load in loads[1:]:
        load.wait()
    active = jnp.broadcast_to(jnp.where(ct[...] > me_w, 1.0, 0.0).astype(F32), (SUB, 128))
    lane_bits = (st.shape[2] - 1).bit_length()

    def received_tiles(v, f):
        other = f ^ 1
        first, stride = FACE_ROWS[other]
        line = jnp.broadcast_to(nb[f : f + 1, :], (SUB, 128))
        slot = line & ((1 << lane_bits) - 1)
        away = (line >> lane_bits) - me_p
        here = away == 0
        before = (away == -1) | (away == planes - 1)

        def take(tile):
            return jnp.take_along_axis(tile, slot, axis=1, mode="promise_in_bounds")

        tiles = []
        for start in FACE_STARTS:
            if stride == 1:
                tile = take(st[v, pl.ds(first + start, SUB), :])
            else:
                tile = take(st[v, pl.ds(first + stride * start, SUB, stride=stride), :])
            if f < 2:
                low = take(halo[v, 0, other, pl.ds(start, SUB), :])
                high = take(halo[v, 1, other, pl.ds(start, SUB), :])
                tile = jnp.where(here, tile, jnp.where(before, low, high))
            tiles.append(tile)
        tiles[-1] = fresh_rows(tiles[-1], FACE - SUB * (len(FACE_STARTS) - 1))
        return tiles

    def residual(v):
        for f in (2, 3, 0, 1):
            if f == 0:
                for side in range(2):
                    for g in range(2):
                        halo_copy(v, side, g).wait_recv()
            tiles = received_tiles(v, f)

            def product(m):
                row = (f * FACE + m) * FACE
                total = fc[pl.ds(row, SUB), :] * tiles[0]
                for t in range(1, len(tiles)):
                    total = total + fc[pl.ds(row + FACE_STARTS[t], SUB), :] * tiles[t]
                return total

            whole = FACE // SUB * SUB
            for m in range(0, whole, SUB):
                fl[f, pl.ds(m, SUB), :] = row_sums([product(m + s) for s in range(SUB)])
            for m in range(whole, FACE):
                fl[f, pl.ds(m, 1), :] = jnp.sum(product(m), axis=0, keepdims=True)
        for f in range(4):
            first, stride = FACE_ROWS[f]
            rows = pl.ds(first, FACE) if stride == 1 else pl.ds(first, FACE, stride=stride)
            r[v, rows, :] = r[v, rows, :] - fl[f, 0:FACE, :]
        total = ssq[...]
        for tile in vector_tiles(lambda start: r[v, pl.ds(start, SUB), :]):
            total = total + tile * tile
        ssq[...] = total

    def forward(v, wall_element):
        if wall_element:
            source = lambda start: r[v, pl.ds(start, SUB), :]
        else:
            for half in range(2):
                fwd_copy(v, half).wait_recv()

            def emit_inner(first, rows):
                inner[pl.ds(first, SUB), :] = r[v, pl.ds(first, SUB), :] - rows

            apply_block(cp, lambda start: below[v, pl.ds(start, SUB), :], emit_inner)
            source = lambda start: inner[pl.ds(start, SUB), :]

        def emit(first, rows):
            w[v, pl.ds(first, SUB), :] = active * rows

        def send(half):
            @pl.when(me_w < top)
            def _():
                fwd_copy(v, half).start()

        apply_block(pv, source, emit, lambda: send(0))
        send(1)

    def send_down(v, source):
        def store(start, rows):
            back[v, pl.ds(start, SUB), :] = rows

        for half, starts in enumerate((STARTS[: GROUPS // 2], STARTS[GROUPS // 2 :])):
            apply_transposed(cp, lambda j: source[v, pl.ds(j, 1), :], store, starts)
            bwd_copy(v, half).start()

    def finish(v, source):
        for start in STARTS:
            rows = pl.ds(start, SUB)
            fresh[v, rows, :] = 0.2 * st[v, rows, :] + 0.8 * source[v, rows, :]
        out_copy(v).start()

    def first_loop(v, carry):
        residual(v)

        @pl.when(me_w == 0)
        def _():
            @pl.when(v == 0)
            def _():
                pivot_load.wait()

            forward(v, True)

        return carry

    lax.fori_loop(0, VARS, first_loop, 0)

    plane_sums[me_p] = ssq[...]
    for d in range(1, planes):
        plane_copy(d).start()

    @pl.when(me_w > 0)
    def _():
        pivot_load.wait()
        coupling_load.wait()

        def second_loop(v, carry):
            forward(v, False)

            @pl.when(me_w == top)
            def _():
                send_down(v, w)

            return carry

        lax.fori_loop(0, VARS, second_loop, 0)

        @pl.when(me_w == top)
        def _():
            for v in range(VARS):
                finish(v, w)

    for d in range(1, planes):
        plane_copy(d).wait()
    total = plane_sums[0]
    for i in range(1, planes):
        total = total + plane_sums[i]
    wall_own[...] = total
    wall_sums[me_w] = total
    for d in range(1, walls):
        wall_copy(d).start()

    @pl.when(me_w < top)
    def _():
        def third_loop(v, carry):
            for half in range(2):
                bwd_copy(v, half).wait_recv()

            def emit(first, rows):
                x[v, pl.ds(first, SUB), :] = active * (w[v, pl.ds(first, SUB), :] - rows)

            apply_block(pv, lambda start: above[v, pl.ds(start, SUB), :], emit)

            @pl.when(me_w > 0)
            def _():
                send_down(v, x)

            finish(v, x)
            return carry

        lax.fori_loop(0, VARS, third_loop, 0)

    for d in range(1, walls):
        wall_copy(d).wait()
    total = wall_sums[0]
    for i in range(1, walls):
        total = total + wall_sums[i]
    mean[0, 0] = jnp.sum(total) / float(VARS * DOFS * 128 * planes * walls)

    def drain(v, carry):
        out_copy(v).wait()
        for side in range(2):
            for f in range(2):
                halo_copy(v, side, f).wait_send()

        @pl.when(me_w < top)
        def _():
            for half in range(2):
                fwd_copy(v, half).wait_send()

        @pl.when(me_w > 0)
        def _():
            for half in range(2):
                bwd_copy(v, half).wait_send()

        return carry

    lax.fori_loop(0, VARS, drain, 0)


def body(planes, walls, state, rhs, pivot_inv, coupling, face_coupling, neighbors, counts):
    lines = state.shape[3]
    assert state.shape[2] == 1 and lines == 128 and walls > 1
    rows = DOFS + 3
    face_rows = FACE + 7
    vectors = pltpu.VMEM((VARS, rows, lines), F32)
    dma = pltpu.SemaphoreType.DMA
    anywhere = pl.BlockSpec(memory_space=pltpu.HBM)
    new_state, mean = pl.pallas_call(
        functools.partial(kernel, planes, walls),
        out_shape=(
            jax.ShapeDtypeStruct(state.shape, F32),
            jax.ShapeDtypeStruct((1, 1), F32),
        ),
        in_specs=[anywhere] * 7,
        out_specs=(anywhere, pl.BlockSpec(memory_space=pltpu.SMEM)),
        scratch_shapes=[
            vectors,
            vectors,
            pltpu.VMEM((DOFS * DOFS, lines), F32),
            pltpu.VMEM((DOFS * DOFS, lines), F32),
            pltpu.VMEM((4 * FACE * FACE, lines), F32),
            pltpu.VMEM((4, lines), jnp.int32),
            pltpu.VMEM((1, lines), jnp.int32),
            pltpu.VMEM((VARS, 2, 2, face_rows, lines), F32),
            pltpu.VMEM((4, face_rows, lines), F32),
            vectors,
            pltpu.VMEM((rows, lines), F32),
            vectors,
            vectors,
            vectors,
            vectors,
            vectors,
            pltpu.VMEM((SUB, lines), F32),
            pltpu.VMEM((planes, SUB, lines), F32),
            pltpu.VMEM((SUB, lines), F32),
            pltpu.VMEM((walls, SUB, lines), F32),
            dma((7,)),
            dma((VARS,)),
            dma((VARS, 2, 2)),
            dma((VARS, 2, 2)),
            dma((VARS, 2)),
            dma((VARS, 2)),
            dma((VARS, 2)),
            dma((VARS, 2)),
            dma((planes,)),
            dma((planes,)),
            dma((walls,)),
            dma((walls,)),
        ],
        compiler_params=pltpu.CompilerParams(
            collective_id=0, has_side_effects=True, vmem_limit_bytes=67_043_328
        ),
        name="line_sweep",
    )(
        state, rhs, pivot_inv, coupling, face_coupling, neighbors.T, counts.reshape(1, lines)
    )
    return new_state, mean.reshape(())


def solution(mesh):
    planes, walls = mesh.shape["plane"], mesh.shape["wall"]
    field = P(None, None, "wall", "plane")
    return jax.shard_map(
        functools.partial(body, planes, walls),
        mesh=mesh,
        in_specs=(
            field, field, field, field,
            P(None, None, None, "wall", "plane"),
            P("plane", None),
            P("plane"),
        ),
        out_specs=(field, P()),
        check_vma=False,
    )
```
